512 devices in a mesh: chaos: 32 (over x, y), slab: 16 (over z, core).
Axes of the slice: x: 4, y: 8, z: 8, core: 2. Of those that a mesh axis runs over, the one named last changes fastest.
Arguments:
- displacement: float32 [288, 3, 12288], P('chaos', None, 'slab'), may hold values from -1.5 to 1.5
- load: float32 [288, 3, 12288], P('chaos', None, 'slab'), may hold values from -12 to 12
- mean_modulus: float32 [12288], P('slab'), may hold values from 0.5 to 2
- modes: float32 [10, 12288], P(None, 'slab'), may hold values from -0.6 to 0.6
- owner: int32 [288], replicated, may hold values from 0 to 287, each once
Outputs:
- solution: float32 [288, 3, 12288], P('chaos', None, 'slab')
- residual: float32 [288, 3, 12288], P('chaos', None, 'slab')
The draws below stay inside these ranges and needn't reach their ends.
Inputs may be any that keep to these rules, and one draw needn't show every extreme that they name: `owner`: each value appears exactly once. Slot s lies on device s // 9 of the chaos axis; values of 286 or more mark empty slots.
All inputs are finite; a program needn't handle non-finite values.
Results may differ from the reference program's by a relative error of at most 0.0003.
Values sent between devices are 32-bit elements; how exact they have to be, the bound alone decides.
A program may use at most 128 MiB of HBM per device.

```python
import math
import jax
import jax.numpy as jnp
import numpy as np

NX = 24
NY = 32
KL = 10
DEG = 3
SWEEPS = 4
ITERS = 2
NZ = 16
SLOTS = 288


def level_of(stream_key, shape, cuts, smallest, high):
    def one(axis_at, shards_of):
        draws = jax.random.uniform(jax.random.fold_in(jax.random.fold_in(stream_key, 6), axis_at), (shards_of,), jnp.float32, smallest / len(cuts), high / len(cuts))
        return jnp.repeat(jnp.exp(draws), shape[axis_at] // shards_of).reshape((-1,) + (1,) * (len(shape) - axis_at - 1))

    factor_of = one(*cuts[0])
    for cut in cuts[1:]:
        factor_of = factor_of * one(*cut)
    return factor_of


def centred(own_key, shape, scale, reach, cuts=(), held_as=jnp.bfloat16):
    drawn = scale * jax.random.normal(own_key, shape, jnp.float32)
    if cuts:
        drawn = drawn * level_of(own_key, shape, cuts, -0.22, 0.18)
    return jnp.clip(drawn, -reach, reach).astype(held_as)


def setup_inputs(seed: int = 0) -> dict:
    seeds = jax.random.split(jax.random.key(seed), 6)
    return {
        "displacement": centred(seeds[0], (SLOTS, 3, NZ * NX * NY), 0.25, 1.5, ((0, 32), (2, 16)), jnp.float32),
        "load": centred(seeds[1], (SLOTS, 3, NZ * NX * NY), 2.0, 12.0, ((0, 32), (2, 16)), jnp.float32),
        "mean_modulus": jnp.clip(jnp.exp(math.log(2.0) - 1.3862944 * jax.random.uniform(seeds[2], (NZ * NX * NY,), jnp.float32) ** level_of(seeds[2], (NZ * NX * NY,), ((0, 16),), -0.2, 0.2)), 0.5, 2.0),
        "modes": centred(seeds[3], (KL, NZ * NX * NY), 0.15, 0.6, ((1, 16),), jnp.float32),
        "owner": jax.random.permutation(seeds[4], SLOTS).astype(jnp.int32),
    }


bound_high = 50.0
bound_low = 2.5

def multi_indices():
    listing = [[]]
    for variable in range(KL):
        extended_list = []
        for prefix in listing:
            for degree in range(DEG + 1 - sum(prefix)):
                extended_list.append(prefix + [degree])
        listing = extended_list
    return listing

def chaos_tables():
    listing = multi_indices()
    lookup = {tuple(multi_entry): number for number, multi_entry in enumerate(listing)}
    number_all = len(listing)
    up_index = np.full((number_all, KL), number_all, np.int32)
    up_weight = np.zeros((number_all, KL), np.float32)
    down_index = np.full((number_all, KL), number_all, np.int32)
    down_weight = np.zeros((number_all, KL), np.float32)
    for number, multi_entry in enumerate(listing):
        for variable in range(KL):
            raised = list(multi_entry)
            raised[variable] += 1
            if tuple(raised) in lookup:
                up_index[number, variable] = lookup[tuple(raised)]
                up_weight[number, variable] = math.sqrt(multi_entry[variable] + 1)
            if multi_entry[variable] > 0:
                lowered = list(multi_entry)
                lowered[variable] -= 1
                down_index[number, variable] = lookup[tuple(lowered)]
                down_weight[number, variable] = math.sqrt(multi_entry[variable])
    return (up_index, up_weight, down_index, down_weight)

def slot_neighbours(owner):
    up_index, up_weight, down_index, down_weight = chaos_tables()
    number_all = up_index.shape[0]
    live_slots = owner < number_all
    clipped = jnp.minimum(owner, number_all - 1)
    inverse = jnp.argsort(owner).astype(jnp.int32)

    def to_slots(index_table, weight_table):
        targets = jnp.asarray(index_table)[clipped]
        present = (targets < number_all) & live_slots[:, None]
        slots_of = inverse[jnp.minimum(targets, number_all - 1)]
        weights = jnp.where(present, jnp.asarray(weight_table)[clipped], 0.0)
        return (jnp.where(present, slots_of, 0).astype(jnp.int32), weights.astype(jnp.float32))
    return (to_slots(up_index, up_weight), to_slots(down_index, down_weight), live_slots)

def plane_masks(length):
    position = jnp.arange(length, dtype=jnp.int32)
    return (position // NY % NX, position % NY)

def forward_flat(values, step_size, keep):
    shifted = jnp.concatenate([values[..., step_size:], jnp.zeros_like(values[..., :step_size])], axis=-1)
    return jnp.where(keep, shifted, 0.0) - values

def backward_flat(values, step_size, keep):
    shifted = jnp.concatenate([jnp.zeros_like(values[..., :step_size]), values[..., :-step_size]], axis=-1)
    return values - jnp.where(keep, shifted, 0.0)

def stiffness_flat(fields, modulus):
    plane_size = NX * NY
    lowered = [field_one[..., :-plane_size] for field_one in fields]
    raised = [field_one[..., plane_size:] for field_one in fields]
    across_x, along_y = plane_masks(lowered[0].shape[-1])
    inner_x, inner_y = plane_masks(lowered[0].shape[-1] - plane_size)

    def slope_of(component, direction):
        if direction == 2:
            return raised[component] - lowered[component]
        if direction == 0:
            return forward_flat(lowered[component], NY, across_x != NX - 1)
        return forward_flat(lowered[component], 1, along_y != NY - 1)
    spread = slope_of(0, 0) + slope_of(1, 1) + slope_of(2, 2)
    results = []
    for component in range(3):
        summed = 0.0
        for direction in range(3):
            gradient = slope_of(component, direction)
            if direction == component:
                gradient = gradient + spread
            flux_term = modulus * gradient
            if direction == 2:
                summed = summed + (flux_term[..., plane_size:] - flux_term[..., :-plane_size])
            elif direction == 0:
                summed = summed + backward_flat(flux_term[..., plane_size:], NY, inner_x != 0)
            else:
                summed = summed + backward_flat(flux_term[..., plane_size:], 1, inner_y != 0)
        results.append(-summed)
    return results

def chebyshev(residual_in, apply_mean):
    center_value = 0.5 * (bound_high + bound_low)
    half_width = 0.5 * (bound_high - bound_low)
    ratio_value = center_value / half_width
    update = residual_in / center_value
    increment = update
    rho_prev = 1.0 / ratio_value
    for sweep_turn in range(SWEEPS):
        rho_next = 1.0 / (2.0 * ratio_value - rho_prev)
        increment = rho_next * rho_prev * increment + 2.0 * rho_next / half_width * (residual_in - apply_mean(update))
        update = update + increment
        rho_prev = rho_next
    return update

def reference(displacement, load, mean_modulus, modes, owner):
    plane_size = NX * NY
    (slot_up, weight_up), (slot_down, weight_down), live_slots = slot_neighbours(owner)
    keep_mask = live_slots[:, None, None]
    solution = jnp.where(keep_mask, displacement, 0.0)
    target = jnp.where(keep_mask, load, 0.0)
    moduli = jnp.concatenate([mean_modulus[None], modes], axis=0)
    moduli_ext = jnp.concatenate([jnp.zeros_like(moduli[:, :plane_size]), moduli], axis=1)

    def stiffness_global(field_in, modulus_ext):
        padded = jnp.pad(field_in, ((0, 0), (0, 0), (plane_size, plane_size)))
        return jnp.stack(stiffness_flat([padded[:, component] for component in range(3)], modulus_ext), axis=1)

    def operator(field_in):
        summed = stiffness_global(jnp.where(live_slots[:, None, None], field_in, 0.0), moduli_ext[0])
        for term_index in range(KL):
            mixed_terms = weight_up[:, term_index][:, None, None] * field_in[slot_up[:, term_index]]
            mixed_terms = mixed_terms + weight_down[:, term_index][:, None, None] * field_in[slot_down[:, term_index]]
            summed = summed + stiffness_global(mixed_terms, moduli_ext[term_index + 1])
        return summed

    def apply_mean(field_in):
        return stiffness_global(field_in, moduli_ext[0])
    residual = target
    for iteration in range(ITERS):
        residual = target - operator(solution)
        solution = solution + chebyshev(residual, apply_mean)
    return (solution, residual)
```

```python
import functools
import heapq
import itertools
import math

import jax
import jax.numpy as jnp
import numpy as np
from jax import lax
from jax.experimental import pallas as pl
from jax.experimental.pallas import tpu as pltpu
from jax.sharding import PartitionSpec as P

NX, NY, KL, DEG, SWEEPS, ITERS = 24, 32, 10, 3, 4, 2
PX, PY = 4, 8
SLOTS_DEV = 9
ROW = 6
PER_SLOT = 3 * ROW
BLOCK = 168
GROUPS = 3
GSLOTS = SLOTS_DEV // GROUPS
GROWS = 56
THETA, DELTA = 26.25, 23.75
MESH = pl.DeviceIdType.MESH
DIRS = {"x+": (1, 0), "x-": (-1, 0), "y+": (0, 1), "y-": (0, -1)}
PIECES = {
    ("A", None): (0, 64),
    ("A", 0): (0, 32),
    ("A", 1): (32, 32),
    ("B", None): (64, 104),
    ("B", 0): (64, 56),
    ("B", 1): (120, 48),
}


def relative(ox, oy):
    return ((ox + PX // 2 - 1) % PX - (PX // 2 - 1), (oy + PY // 2 - 1) % PY - (PY // 2 - 1))


def gather_plan():
    count = itertools.count()
    halves = {}

    def allowed(way, part, owner, half):
        sends = []
        first, second = ("x", "y") if part == "A" else ("y", "x")
        at = {"x": owner[0], "y": owner[1]}
        far = {"x": PX // 2, "y": PY // 2}

        def chain(axis):
            reach, last = abs(at[axis]), far[axis] - 1
            if reach < last:
                sends.append((way, part, owner, None))
            elif reach == last:
                sends.append((way, part, owner, 0 if way[1] == "+" else 1))

        chain(way[0])
        if way[0] == first:
            ready = half is None
            if not ready:
                halves[part, owner] = halves.get((part, owner), 0) + 1
                ready = halves[part, owner] == 2
            if ready:
                sends.append((second + "+", part, owner, None))
                sends.append((second + "-", part, owner, None))
        return sends

    start = [(d, p, (0, 0), None) for p, d in (("A", "x+"), ("B", "y+"), ("A", "x-"), ("B", "y-"))]
    start += [(d, p, (0, 0), None) for p, d in (("A", "y+"), ("B", "x+"), ("A", "y-"), ("B", "x-"))]
    queues, busy, events, arrivals = {d: [] for d in DIRS}, dict.fromkeys(DIRS, False), [], []

    def begin(way, now):
        if queues[way] and not busy[way]:
            message = queues[way].pop(0)
            busy[way] = True
            took = PIECES[message[1], message[3]][1] / 91.0
            heapq.heappush(events, (now + took, next(count), "sent", message))
            heapq.heappush(events, (now + took + 2.0, next(count), "here", message))

    for message in start:
        queues[message[0]].append(message)
    for way in DIRS:
        begin(way, 0.0)
    while events:
        now, _, kind, message = heapq.heappop(events)
        way, part, owner, half = message
        if kind == "sent":
            busy[way] = False
        else:
            owner = relative(owner[0] - DIRS[way][0], owner[1] - DIRS[way][1])
            sends = allowed(way, part, owner, half)
            arrivals.append(((way, part, owner, half), sends))
            for send in sends:
                queues[send[0]].append(send)
        for each in DIRS:
            begin(each, now)
    return start, arrivals


def multi_indices():
    listing = [[]]
    for variable in range(KL):
        extended = []
        for prefix in listing:
            for degree in range(DEG + 1 - sum(prefix)):
                extended.append(prefix + [degree])
        listing = extended
    return listing


def chaos_tables(slots_all):
    listing = multi_indices()
    lookup = {tuple(entry): number for number, entry in enumerate(listing)}
    targets = np.full((2 * KL, slots_all), -1, np.int32)
    weights = np.zeros((2 * KL, slots_all), np.float32)
    for number, entry in enumerate(listing):
        for variable in range(KL):
            for side, step in ((0, 1), (1, -1)):
                other = list(entry)
                other[variable] += step
                if tuple(other) in lookup:
                    targets[side * KL + variable, number] = lookup[tuple(other)]
                    weights[side * KL + variable, number] = math.sqrt(
                        max(entry[variable], other[variable])
                    )
    return len(listing), targets, weights


def neighbour_tables(owner):
    slots_all = owner.shape[0]
    number_all, targets, weights = chaos_tables(slots_all)
    own = lax.dynamic_slice_in_dim(owner, lax.axis_index("chaos") * SLOTS_DEV, SLOTS_DEV, 0)
    numbers = jnp.arange(slots_all, dtype=jnp.int32)
    chosen = own[:, None, None] == numbers
    target = jnp.sum(jnp.where(chosen, jnp.asarray(targets), 0), axis=-1)
    weight = jnp.sum(jnp.where(chosen, jnp.asarray(weights), 0.0), axis=-1)
    rows = (numbers // SLOTS_DEV) * BLOCK + (numbers % SLOTS_DEV) * PER_SLOT
    row = jnp.sum(jnp.where(target[:, :, None] == owner, rows, 0), axis=-1)
    live = jnp.where(own < number_all, 1.0, 0.0)
    return row, jnp.concatenate([weight, live[:, None]], axis=1)


def kernel(
    rows_ref,
    weight_ref,
    disp_ref,
    load_ref,
    moduli_ref,
    sol_ref,
    res_ref,
    gathered_0,
    gathered_1,
    u_ref,
    f_ref,
    r_ref,
    z_ref,
    p_ref,
    t_ref,
    mod,
    mod_low,
    mod_x,
    mod_y,
    up_out,
    down_out,
    up_in,
    down_in,
    ag_send,
    ag_recv,
    up_send,
    up_recv,
    down_send,
    down_recv,
    mod_send,
    mod_recv,
):
    chaos = lax.axis_index("chaos")
    slab = lax.axis_index("slab")
    slabs = lax.axis_size("slab")
    cx, cy = chaos // PY, chaos % PY
    has_low, has_high = slab > 0, slab < slabs - 1

    def chaos_at(dx, dy):
        return lax.rem(cx + dx + PX, PX) * PY + lax.rem(cy + dy + PY, PY)

    lane = lax.broadcasted_iota(jnp.int32, (8, 128), 1)
    sub = lax.broadcasted_iota(jnp.int32, (8, 128), 0)
    inside = sub < ROW
    first_y = lane % NY == 0
    zero = jnp.zeros((8, 128), jnp.float32)

    def up_x(f):
        rolled = pltpu.roll(f, 128 - NY, 1)
        return jnp.where(lane < 128 - NY, rolled, pltpu.roll(rolled, 7, 0))

    def down_x(f):
        rolled = pltpu.roll(f, NY, 1)
        return jnp.where(lane < NY, pltpu.roll(rolled, 1, 0), rolled)

    def up_y(f):
        return pltpu.roll(f, 127, 1)

    def down_y(f):
        return jnp.where(first_y, 0.0, pltpu.roll(f, 1, 1))

    barrier = pltpu.get_barrier_semaphore()
    for dx, dy in DIRS.values():
        pl.semaphore_signal(
            barrier, inc=1, device_id=(chaos_at(dx, dy), slab), device_id_type=MESH
        )

    @pl.when(has_low)
    def _():
        pl.semaphore_signal(barrier, inc=1, device_id=(chaos, slab - 1), device_id_type=MESH)

    @pl.when(has_high)
    def _():
        pl.semaphore_signal(barrier, inc=1, device_id=(chaos, slab + 1), device_id_type=MESH)

    for ref in (u_ref, z_ref):
        ref[BLOCK - 8 : BLOCK, :] = zero

    def take(s, _):
        live = weight_ref[s, 2 * KL]
        for c in range(3):
            for k in range(ROW):
                at = pl.ds(s * PER_SLOT + c * ROW + k, 1)
                piece = disp_ref[s, c : c + 1, 128 * k : 128 * k + 128]
                u_ref[at, :] = jnp.where(live > 0.5, piece, 0.0)
                piece = load_ref[s, c : c + 1, 128 * k : 128 * k + 128]
                f_ref[at, :] = jnp.where(live > 0.5, piece, 0.0)
        return 0

    lax.fori_loop(0, SLOTS_DEV, take, 0)
    for v in range(KL + 1):
        mod[v] = zero
        for k in range(ROW):
            mod[v, k : k + 1, :] = moduli_ref[v : v + 1, 128 * k : 128 * k + 128]

    @pl.when(jnp.logical_not(has_low))
    def _():
        for v in range(KL + 1):
            mod_low[v] = zero

        def clear(i, _):
            up_in[i] = jnp.zeros((GROWS, 128), jnp.float32)
            return 0

        lax.fori_loop(0, ITERS * (SWEEPS + 1) * GROUPS, clear, 0)

    @pl.when(jnp.logical_not(has_high))
    def _():
        def clear(i, _):
            down_in[i] = jnp.zeros((GROWS, 128), jnp.float32)
            return 0

        lax.fori_loop(0, ITERS * (SWEEPS + 1) * GROUPS, clear, 0)

    neighbours = len(DIRS) + has_low.astype(jnp.int32) + has_high.astype(jnp.int32)
    pl.semaphore_wait(barrier, neighbours)

    mod_copy = pltpu.make_async_remote_copy(
        src_ref=mod,
        dst_ref=mod_low,
        send_sem=mod_send,
        recv_sem=mod_recv,
        device_id=(chaos, slab + 1),
        device_id_type=MESH,
    )

    @pl.when(has_high)
    def _():
        mod_copy.start()

    blocks = (gathered_0, gathered_1)
    start, arrivals = gather_plan()
    ids = {arrival: number for number, (arrival, _) in enumerate(arrivals)}

    def gather_copy(turn, way, part, owner, half):
        dx, dy = DIRS[way]
        number = ids[way, part, relative(owner[0] - dx, owner[1] - dy), half]
        first, size = PIECES[part, half]
        base = chaos_at(*owner) * BLOCK + first
        piece = blocks[turn].at[pl.ds(pl.multiple_of(base, 8), size)]
        return pltpu.make_async_remote_copy(
            src_ref=piece,
            dst_ref=piece,
            send_sem=ag_send.at[turn, number],
            recv_sem=ag_recv.at[turn, number],
            device_id=(chaos_at(dx, dy), slab),
            device_id_type=MESH,
        )

    def exchange(turn, k, g):
        i = (turn * (SWEEPS + 1) + k) * GROUPS + g
        up = pltpu.make_async_remote_copy(
            src_ref=up_out.at[i],
            dst_ref=up_in.at[i],
            send_sem=up_send.at[i],
            recv_sem=up_recv.at[i],
            device_id=(chaos, slab + 1),
            device_id_type=MESH,
        )
        down = pltpu.make_async_remote_copy(
            src_ref=down_out.at[i],
            dst_ref=down_in.at[i],
            send_sem=down_send.at[i],
            recv_sem=down_recv.at[i],
            device_id=(chaos, slab - 1),
            device_id_type=MESH,
        )
        return i, up, down

    def send(turn, k, g):
        _, up, down = exchange(turn, k, g)

        @pl.when(has_high)
        def _():
            up.start()

        @pl.when(has_low)
        def _():
            down.start()

    def receive(turn, k, g):
        _, up, down = exchange(turn, k, g)

        @pl.when(has_low)
        def _():
            up.wait_recv()

        @pl.when(has_high)
        def _():
            down.wait_recv()

    def sent(turn, k, g):
        _, up, down = exchange(turn, k, g)

        @pl.when(has_high)
        def _():
            up.wait_send()

        @pl.when(has_low)
        def _():
            down.wait_send()

    def own_part(i, g, j, at, x, y, z):
        px, py = [up_x(e) for e in x], [up_y(e) for e in y]
        spread = (px[0] - at[0]) + (py[1] - at[1]) - at[2]
        flux_x = [px[c] - at[c] for c in range(3)]
        flux_y = [py[c] - at[c] for c in range(3)]
        flux_x[0] = flux_x[0] + spread
        flux_y[1] = flux_y[1] + spread
        base = (g * GSLOTS + j) * PER_SLOT
        for c in range(3):
            total = (flux_x[c] - down_x(flux_x[c])) + (flux_y[c] - down_y(flux_y[c]))
            total = total - at[c] - z[c]
            if c == 2:
                total = total + spread - z[c]
            t_ref[pl.ds(base + c * ROW, ROW), :] = total[:ROW]
            low = at[c] if c < 2 else at[c] - spread
            inner = pl.ds(j * PER_SLOT + c * ROW, ROW)
            up_out[i, inner, :] = low[:ROW]
            down_out[i, inner, :] = z[c][:ROW]

    def minus_image(i, g, j):
        base = (g * GSLOTS + j) * PER_SLOT
        low = [up_in[i, pl.ds(j * PER_SLOT + c * ROW, 8), :] for c in range(3)]
        high = [down_in[i, pl.ds(j * PER_SLOT + c * ROW, 8), :] for c in range(3)]
        across = jnp.where(inside, high[2], 0.0)
        own = [t_ref[pl.ds(base + c * ROW, 8), :] for c in range(3)]
        return [
            own[0] + (across - down_x(across)) + high[0] + low[0],
            own[1] + (across - down_y(across)) + high[1] + low[1],
            own[2] + 2.0 * across + low[2],
        ]

    def slot_rows(g, j, c, size):
        return pl.ds((g * GSLOTS + j) * PER_SLOT + c * ROW, size)

    def mean_part(turn, k, g, j, z):
        i, _, _ = exchange(turn, k, g)
        own_part(
            i,
            g,
            j,
            [mod[0] * e for e in z],
            [mod_x[0] * e for e in z],
            [mod_y[0] * e for e in z],
            [mod_low[0] * e for e in z],
        )

    ratio = THETA / DELTA
    rho = 1.0 / ratio
    factors = []
    for _ in range(SWEEPS):
        rho_next = 1.0 / (2.0 * ratio - rho)
        factors.append((rho_next * rho, 2.0 * rho_next / DELTA))
        rho = rho_next

    def iteration(turn):
        gathered = blocks[turn]
        gathered[pl.ds(pl.multiple_of(chaos * BLOCK, 8), BLOCK), :] = u_ref[...]
        for message in start:
            gather_copy(turn, *message).start()

        if turn == 0:

            @pl.when(has_low)
            def _():
                mod_copy.wait_recv()

            for v in range(KL + 1):
                mod_x[v] = jnp.where(inside, down_x(mod[v]), 0.0)
                mod_y[v] = down_y(mod[v])

        for (way, part, owner, half), sends in arrivals:
            dx, dy = DIRS[way]
            first, size = PIECES[part, half]
            base = chaos_at(*owner) * BLOCK + first
            piece = blocks[turn].at[pl.ds(pl.multiple_of(base, 8), size)]
            number = ids[way, part, owner, half]
            pltpu.make_async_remote_copy(
                src_ref=piece,
                dst_ref=piece,
                send_sem=ag_send.at[turn, number],
                recv_sem=ag_recv.at[turn, number],
                device_id=(chaos_at(dx, dy), slab),
                device_id_type=MESH,
            ).wait_recv()
            for message in sends:
                gather_copy(turn, *message).start()

        def couple(g, _):
            i, _, _ = exchange(turn, 0, g)
            for j in range(GSLOTS):
                s = g * GSLOTS + j
                u = [u_ref[slot_rows(g, j, c, 8), :] for c in range(3)]
                at = [mod[0] * e for e in u]
                x = [mod_x[0] * e for e in u]
                y = [mod_y[0] * e for e in u]
                z = [mod_low[0] * e for e in u]
                for v in range(1, KL + 1):
                    up_row = rows_ref[s, v - 1]
                    down_row = rows_ref[s, KL + v - 1]
                    up_weight, down_weight = weight_ref[s, v - 1], weight_ref[s, KL + v - 1]
                    m, mx, my, mz = mod[v], mod_x[v], mod_y[v], mod_low[v]
                    for c in range(3):
                        e = up_weight * gathered[pl.ds(up_row + c * ROW, 8), :]
                        e = e + down_weight * gathered[pl.ds(down_row + c * ROW, 8), :]
                        at[c] = at[c] + m * e
                        x[c] = x[c] + mx * e
                        y[c] = y[c] + my * e
                        z[c] = z[c] + mz * e
                own_part(i, g, j, at, x, y, z)
            send(turn, 0, g)
            return 0

        lax.fori_loop(0, GROUPS, couple, 0)

        def first_update(g, _):
            receive(turn, 0, g)
            i, _, _ = exchange(turn, 0, g)
            for j in range(GSLOTS):
                image = minus_image(i, g, j)
                starts = []
                for c in range(3):
                    r = f_ref[slot_rows(g, j, c, 8), :] + image[c]
                    z = r * (1.0 / THETA)
                    rows = slot_rows(g, j, c, ROW)
                    r_ref[rows, :] = r[:ROW]
                    z_ref[rows, :] = z[:ROW]
                    p_ref[rows, :] = z[:ROW]
                    starts.append(jnp.where(inside, z, 0.0))
                mean_part(turn, 1, g, j, starts)
            send(turn, 1, g)
            return 0

        lax.fori_loop(0, GROUPS, first_update, 0)

        for k in range(1, SWEEPS + 1):
            keep, gain = factors[k - 1]

            def sweep(g, _, k=k, keep=keep, gain=gain):
                receive(turn, k, g)
                i, _, _ = exchange(turn, k, g)
                for j in range(GSLOTS):
                    image = minus_image(i, g, j)
                    updated = []
                    for c in range(3):
                        whole, rows = slot_rows(g, j, c, 8), slot_rows(g, j, c, ROW)
                        p = keep * p_ref[whole, :] + gain * (r_ref[whole, :] + image[c])
                        z = z_ref[whole, :] + p
                        if k < SWEEPS:
                            p_ref[rows, :] = p[:ROW]
                            z_ref[rows, :] = z[:ROW]
                            updated.append(jnp.where(inside, z, 0.0))
                        else:
                            u_ref[rows, :] = (u_ref[whole, :] + z)[:ROW]
                    if k < SWEEPS:
                        mean_part(turn, k + 1, g, j, updated)
                if k < SWEEPS:
                    send(turn, k + 1, g)
                return 0

            lax.fori_loop(0, GROUPS, sweep, 0)

    for turn in range(ITERS):
        iteration(turn)

    def give(s, _):
        for c in range(3):
            for k in range(ROW):
                at = pl.ds(s * PER_SLOT + c * ROW + k, 1)
                sol_ref[s, c : c + 1, 128 * k : 128 * k + 128] = u_ref[at, :]
                res_ref[s, c : c + 1, 128 * k : 128 * k + 128] = r_ref[at, :]
        return 0

    lax.fori_loop(0, SLOTS_DEV, give, 0)

    @pl.when(has_high)
    def _():
        mod_copy.wait_send()

    for turn in range(ITERS):
        for message in start:
            gather_copy(turn, *message).wait_send()
        for _, sends in arrivals:
            for message in sends:
                gather_copy(turn, *message).wait_send()
        for k in range(SWEEPS + 1):
            for g in range(GROUPS):
                sent(turn, k, g)


def per_device(displacement, load, mean_modulus, modes, owner):
    rows, weights = neighbour_tables(owner)
    moduli = jnp.concatenate([mean_modulus[None], modes], axis=0)
    _, arrivals = gather_plan()
    messages = len(arrivals)
    exchanges = ITERS * (SWEEPS + 1) * GROUPS
    field = pltpu.VMEM((BLOCK, 128), jnp.float32)
    moduli_field = pltpu.VMEM((KL + 1, 8, 128), jnp.float32)
    planes = pltpu.VMEM((exchanges, GROWS, 128), jnp.float32)
    out = jax.ShapeDtypeStruct(displacement.shape, jnp.float32)
    smem, vmem = pl.BlockSpec(memory_space=pltpu.SMEM), pl.BlockSpec(memory_space=pltpu.VMEM)
    dma = pltpu.SemaphoreType.DMA
    return pl.pallas_call(
        kernel,
        out_shape=(out, out),
        in_specs=[smem, smem, vmem, vmem, vmem],
        out_specs=(vmem, vmem),
        scratch_shapes=[
            pltpu.VMEM((PX * PY * BLOCK, 128), jnp.float32),
            pltpu.VMEM((PX * PY * BLOCK, 128), jnp.float32),
            field,
            field,
            field,
            field,
            field,
            field,
            moduli_field,
            moduli_field,
            moduli_field,
            moduli_field,
            planes,
            planes,
            planes,
            planes,
            dma((ITERS, messages)),
            dma((ITERS, messages)),
            dma((exchanges,)),
            dma((exchanges,)),
            dma((exchanges,)),
            dma((exchanges,)),
            dma,
            dma,
        ],
        compiler_params=pltpu.CompilerParams(collective_id=0, has_side_effects=True),
        name="galerkin",
    )(rows, weights, displacement, load, moduli)


def solution(mesh):
    in_specs = (P("chaos", None, "slab"), P("chaos", None, "slab"), P("slab"), P(None, "slab"), P())
    out_specs = (P("chaos", None, "slab"), P("chaos", None, "slab"))
    return jax.shard_map(
        per_device, mesh=mesh, in_specs=in_specs, out_specs=out_specs, check_vma=False
    )
```

```python
import functools
import heapq
import itertools
import math

import jax
import jax.numpy as jnp
import numpy as np
from jax import lax
from jax.experimental import pallas as pl
from jax.experimental.pallas import tpu as pltpu
from jax.sharding import PartitionSpec as P

NX, NY, KL, DEG, SWEEPS, ITERS = 24, 32, 10, 3, 4, 2
PX, PY = 4, 8
SLOTS_DEV = 9
ROW = 6
PER_SLOT = 3 * ROW
BLOCK = 168
GROUPS = 3
GSLOTS = SLOTS_DEV // GROUPS
GROWS = 56
THETA, DELTA = 26.25, 23.75
MESH = pl.DeviceIdType.MESH
DIRS = {"x+": (1, 0), "x-": (-1, 0), "y+": (0, 1), "y-": (0, -1)}
CHUNKS = (("x", 0, 64, 32), ("y", 64, 104, 56))
MODES = {("x", 0): "leap", ("y", 0): "leap", ("x", 1): "chain", ("y", 1): "chain"}
LATENCY, HOP, RATE, AHEAD = 2.8, 0.8, 88.0, 1.2


def piece_rows(chunk, half):
    _, first, size, upper = CHUNKS[chunk]
    return {None: (first, size), 0: (first, upper), 1: (first + upper, size - upper)}[half]


def relative(ox, oy):
    return ((ox + PX // 2 - 1) % PX - (PX // 2 - 1), (oy + PY // 2 - 1) % PY - (PY // 2 - 1))


def onward(axis, stage, reach):
    far = (PX if axis == "x" else PY) // 2
    if MODES[axis, stage] == "chain":
        return [(1, reach == far - 1)] if reach < far else []
    if far == 2:
        return [(1, False), (2, True)] if reach == 0 else []
    return {0: [(1, False), (2, False)], 2: [(1, False), (2, True)]}.get(reach, [])


def depth(axis, stage, reach):
    return max((1 + depth(axis, stage, reach + hops) for hops, _ in onward(axis, stage, reach)), default=0)


def gather_plan():
    count = itertools.count()
    halves = {}

    def carried(way, chunk, owner, stage):
        reach = abs(owner["xy".index(way[0])])
        return [
            (way, hops, chunk, owner, (0 if way[1] == "+" else 1) if half else None)
            for hops, half in onward(way[0], stage, reach)
        ]

    def allowed(way, chunk, owner, half):
        first = CHUNKS[chunk][0]
        if way[0] != first:
            return carried(way, chunk, owner, 1)
        sends = carried(way, chunk, owner, 0) if half is None else []
        if half is not None:
            halves[chunk, owner] = halves.get((chunk, owner), 0) + 1
        if half is None or halves[chunk, owner] == 2:
            second = "y" if first == "x" else "x"
            for sign in "+-":
                sends += carried(second + sign, chunk, owner, 1)
        return sends

    def urgency(message):
        way, hops, chunk, owner, _ = message
        axis, first = way[0], CHUNKS[chunk][0]
        reach = abs(owner["xy".index(axis)]) + hops
        if axis != first:
            return -depth(axis, 1, reach)
        return -depth(axis, 0, reach) - depth("y" if axis == "x" else "x", 1, 0)

    queues, busy = {d: [] for d in DIRS}, dict.fromkeys(DIRS, False)
    events, steps = [], []

    def put(message, now):
        heapq.heappush(queues[message[0]], (urgency(message), next(count), message, now))

    def begin(way, now):
        if queues[way] and not busy[way]:
            _, _, message, since = heapq.heappop(queues[way])
            busy[way] = True
            steps.append((max(since, now - AHEAD), next(count), "send", message))
            hops = message[1]
            took = hops * piece_rows(message[2], message[4])[1] / RATE
            heapq.heappush(events, (now + took, next(count), "sent", message))
            here = now + took + LATENCY + HOP * (hops - 1)
            heapq.heappush(events, (here, next(count), "here", message))

    for stage in (0, 1):
        for sign in "+-":
            for chunk, (first, *_) in enumerate(CHUNKS):
                axis = first if stage == 0 else "y" if first == "x" else "x"
                for message in carried(axis + sign, chunk, (0, 0), stage):
                    put(message, 0.0)
    for way in DIRS:
        begin(way, 0.0)
    while events:
        now, _, kind, message = heapq.heappop(events)
        way, hops, chunk, owner, half = message
        if kind == "sent":
            busy[way] = False
        else:
            dx, dy = DIRS[way]
            owner = relative(owner[0] - dx * hops, owner[1] - dy * hops)
            steps.append((now, next(count), "wait", (way, hops, chunk, owner, half)))
            for message in allowed(way, chunk, owner, half):
                put(message, now)
        for each in DIRS:
            begin(each, now)
    return [(kind, message) for _, _, kind, message in sorted(steps)]


def multi_indices():
    listing = [[]]
    for variable in range(KL):
        extended = []
        for prefix in listing:
            for degree in range(DEG + 1 - sum(prefix)):
                extended.append(prefix + [degree])
        listing = extended
    return listing


def chaos_tables(slots_all):
    listing = multi_indices()
    lookup = {tuple(entry): number for number, entry in enumerate(listing)}
    targets = np.full((2 * KL, slots_all), -1, np.int32)
    weights = np.zeros((2 * KL + 1, slots_all), np.float32)
    weights[2 * KL, : len(listing)] = 1.0
    for number, entry in enumerate(listing):
        for variable in range(KL):
            for side, step in ((0, 1), (1, -1)):
                other = list(entry)
                other[variable] += step
                if tuple(other) in lookup:
                    targets[side * KL + variable, number] = lookup[tuple(other)]
                    weights[side * KL + variable, number] = math.sqrt(
                        max(entry[variable], other[variable])
                    )
    return targets, weights


def neighbour_tables(owner):
    slots_all = owner.shape[0]
    targets, weights = chaos_tables(slots_all)
    own = lax.dynamic_slice_in_dim(owner, lax.axis_index("chaos") * SLOTS_DEV, SLOTS_DEV, 0)
    numbers = jnp.arange(slots_all, dtype=jnp.int32)
    chosen = own[:, None, None] == numbers
    target = jnp.sum(jnp.where(chosen, jnp.asarray(targets), 0), axis=-1)
    weight = jnp.sum(jnp.where(chosen, jnp.asarray(weights), 0.0), axis=-1)
    rows = (numbers // SLOTS_DEV) * BLOCK + (numbers % SLOTS_DEV) * PER_SLOT
    row = jnp.sum(jnp.where(target[:, :, None] == owner, rows, 0), axis=-1)
    return row, weight


def kernel(
    rows_ref,
    weight_ref,
    disp_ref,
    load_ref,
    mean_ref,
    modes_ref,
    sol_ref,
    res_ref,
    gathered_0,
    gathered_1,
    u_ref,
    f_ref,
    r_ref,
    z_ref,
    p_ref,
    t_ref,
    mod,
    mod_low,
    mod_x,
    mod_y,
    up_out,
    down_out,
    up_in,
    down_in,
    ag_send,
    ag_recv,
    up_send,
    up_recv,
    down_send,
    down_recv,
    mod_send,
    mod_recv,
):
    chaos = lax.axis_index("chaos")
    slab = lax.axis_index("slab")
    slabs = lax.axis_size("slab")
    cx, cy = chaos // PY, chaos % PY
    has_low, has_high = slab > 0, slab < slabs - 1

    def chaos_at(dx, dy):
        return lax.rem(cx + dx + PX, PX) * PY + lax.rem(cy + dy + PY, PY)

    lane = lax.broadcasted_iota(jnp.int32, (8, 128), 1)
    sub = lax.broadcasted_iota(jnp.int32, (8, 128), 0)
    inside = sub < ROW
    first_y = lane % NY == 0
    zero = jnp.zeros((8, 128), jnp.float32)

    def up_x(f):
        rolled = pltpu.roll(f, 128 - NY, 1)
        return jnp.where(lane < 128 - NY, rolled, pltpu.roll(rolled, 7, 0))

    def down_x(f):
        rolled = pltpu.roll(f, NY, 1)
        return jnp.where(lane < NY, pltpu.roll(rolled, 1, 0), rolled)

    def up_y(f):
        return pltpu.roll(f, 127, 1)

    def down_y(f):
        return jnp.where(first_y, 0.0, pltpu.roll(f, 1, 1))

    barrier = pltpu.get_barrier_semaphore()
    peers = [*DIRS.values(), (2, 0), (0, 2), (0, -2)]
    for dx, dy in peers:
        pl.semaphore_signal(
            barrier, inc=1, device_id=(chaos_at(dx, dy), slab), device_id_type=MESH
        )

    @pl.when(has_low)
    def _():
        pl.semaphore_signal(barrier, inc=1, device_id=(chaos, slab - 1), device_id_type=MESH)

    @pl.when(has_high)
    def _():
        pl.semaphore_signal(barrier, inc=1, device_id=(chaos, slab + 1), device_id_type=MESH)

    for ref in (u_ref, z_ref):
        ref[BLOCK - 8 : BLOCK, :] = zero

    def take(s, _):
        live = weight_ref[s, 2 * KL]
        for c in range(3):
            for k in range(ROW):
                at = pl.ds(s * PER_SLOT + c * ROW + k, 1)
                piece = disp_ref[s, c : c + 1, 128 * k : 128 * k + 128]
                u_ref[at, :] = jnp.where(live > 0.5, piece, 0.0)
                piece = load_ref[s, c : c + 1, 128 * k : 128 * k + 128]
                f_ref[at, :] = jnp.where(live > 0.5, piece, 0.0)
        return 0

    lax.fori_loop(0, SLOTS_DEV, take, 0)
    for v in range(KL + 1):
        mod[v] = zero
        for k in range(ROW):
            nodes = slice(128 * k, 128 * k + 128)
            if v == 0:
                mod[0, k, :] = mean_ref[nodes]
            else:
                mod[v, k : k + 1, :] = modes_ref[v - 1 : v, nodes]

    @pl.when(jnp.logical_not(has_low))
    def _():
        for v in range(KL + 1):
            mod_low[v] = zero

        def clear(i, _):
            up_in[i] = jnp.zeros((GROWS, 128), jnp.float32)
            return 0

        lax.fori_loop(0, ITERS * (SWEEPS + 1) * GROUPS, clear, 0)

    @pl.when(jnp.logical_not(has_high))
    def _():
        def clear(i, _):
            down_in[i] = jnp.zeros((GROWS, 128), jnp.float32)
            return 0

        lax.fori_loop(0, ITERS * (SWEEPS + 1) * GROUPS, clear, 0)

    neighbours = len(peers) + has_low.astype(jnp.int32) + has_high.astype(jnp.int32)
    pl.semaphore_wait(barrier, neighbours)

    mod_copy = pltpu.make_async_remote_copy(
        src_ref=mod,
        dst_ref=mod_low,
        send_sem=mod_send,
        recv_sem=mod_recv,
        device_id=(chaos, slab + 1),
        device_id_type=MESH,
    )

    @pl.when(has_high)
    def _():
        mod_copy.start()

    blocks = (gathered_0, gathered_1)
    steps = gather_plan()
    waits = [message for kind, message in steps if kind == "wait"]
    ids = {message: number for number, message in enumerate(waits)}

    def gather_copy(turn, kind, message):
        way, hops, chunk, owner, half = message
        dx, dy = (hops * d for d in DIRS[way])
        if kind == "send":
            message = (way, hops, chunk, relative(owner[0] - dx, owner[1] - dy), half)
        number = ids[message]
        first, size = piece_rows(chunk, half)
        base = chaos_at(*owner) * BLOCK + first
        piece = blocks[turn].at[pl.ds(pl.multiple_of(base, 8), size)]
        return pltpu.make_async_remote_copy(
            src_ref=piece,
            dst_ref=piece,
            send_sem=ag_send.at[turn, number],
            recv_sem=ag_recv.at[turn, number],
            device_id=(chaos_at(dx, dy), slab),
            device_id_type=MESH,
        )

    def exchange(turn, k, g):
        i = (turn * (SWEEPS + 1) + k) * GROUPS + g
        up = pltpu.make_async_remote_copy(
            src_ref=up_out.at[i],
            dst_ref=up_in.at[i],
            send_sem=up_send.at[i],
            recv_sem=up_recv.at[i],
            device_id=(chaos, slab + 1),
            device_id_type=MESH,
        )
        down = pltpu.make_async_remote_copy(
            src_ref=down_out.at[i],
            dst_ref=down_in.at[i],
            send_sem=down_send.at[i],
            recv_sem=down_recv.at[i],
            device_id=(chaos, slab - 1),
            device_id_type=MESH,
        )
        return i, up, down

    def send(turn, k, g):
        _, up, down = exchange(turn, k, g)

        @pl.when(has_high)
        def _():
            up.start()

        @pl.when(has_low)
        def _():
            down.start()

    def receive(turn, k, g):
        _, up, down = exchange(turn, k, g)

        @pl.when(has_low)
        def _():
            up.wait_recv()

        @pl.when(has_high)
        def _():
            down.wait_recv()

    def sent(turn, k, g):
        _, up, down = exchange(turn, k, g)

        @pl.when(has_high)
        def _():
            up.wait_send()

        @pl.when(has_low)
        def _():
            down.wait_send()

    def own_part(i, g, j, at, x, y, z):
        px, py = [up_x(e) for e in x], [up_y(e) for e in y]
        spread = (px[0] - at[0]) + (py[1] - at[1]) - at[2]
        flux_x = [px[c] - at[c] for c in range(3)]
        flux_y = [py[c] - at[c] for c in range(3)]
        flux_x[0] = flux_x[0] + spread
        flux_y[1] = flux_y[1] + spread
        base = (g * GSLOTS + j) * PER_SLOT
        for c in range(3):
            total = (flux_x[c] - down_x(flux_x[c])) + (flux_y[c] - down_y(flux_y[c]))
            total = total - at[c] - z[c]
            if c == 2:
                total = total + spread - z[c]
            t_ref[pl.ds(base + c * ROW, ROW), :] = total[:ROW]
            low = at[c] if c < 2 else at[c] - spread
            inner = pl.ds(j * PER_SLOT + c * ROW, ROW)
            up_out[i, inner, :] = low[:ROW]
            down_out[i, inner, :] = z[c][:ROW]

    def minus_image(i, g, j):
        base = (g * GSLOTS + j) * PER_SLOT
        low = [up_in[i, pl.ds(j * PER_SLOT + c * ROW, 8), :] for c in range(3)]
        high = [down_in[i, pl.ds(j * PER_SLOT + c * ROW, 8), :] for c in range(3)]
        across = jnp.where(inside, high[2], 0.0)
        own = [t_ref[pl.ds(base + c * ROW, 8), :] for c in range(3)]
        return [
            own[0] + (across - down_x(across)) + high[0] + low[0],
            own[1] + (across - down_y(across)) + high[1] + low[1],
            own[2] + 2.0 * across + low[2],
        ]

    def slot_rows(g, j, c, size):
        return pl.ds((g * GSLOTS + j) * PER_SLOT + c * ROW, size)

    def mean_part(turn, k, g, j, z):
        i, _, _ = exchange(turn, k, g)
        own_part(
            i,
            g,
            j,
            [mod[0] * e for e in z],
            [mod_x[0] * e for e in z],
            [mod_y[0] * e for e in z],
            [mod_low[0] * e for e in z],
        )

    ratio = THETA / DELTA
    rho = 1.0 / ratio
    factors = []
    for _ in range(SWEEPS):
        rho_next = 1.0 / (2.0 * ratio - rho)
        factors.append((rho_next * rho, 2.0 * rho_next / DELTA))
        rho = rho_next

    def iteration(turn):
        gathered = blocks[turn]
        gathered[pl.ds(pl.multiple_of(chaos * BLOCK, 8), BLOCK), :] = u_ref[...]
        began = steps.index(next(step for step in steps if step[0] == "wait"))
        for kind, message in steps[:began]:
            gather_copy(turn, kind, message).start()

        if turn == 0:

            @pl.when(has_low)
            def _():
                mod_copy.wait_recv()

            for v in range(KL + 1):
                mod_x[v] = jnp.where(inside, down_x(mod[v]), 0.0)
                mod_y[v] = down_y(mod[v])

        for kind, message in steps[began:]:
            if kind == "send":
                gather_copy(turn, kind, message).start()
            else:
                gather_copy(turn, kind, message).wait_recv()

        def couple(g, _):
            i, _, _ = exchange(turn, 0, g)
            for j in range(GSLOTS):
                s = g * GSLOTS + j
                u = [u_ref[slot_rows(g, j, c, 8), :] for c in range(3)]
                at = [mod[0] * e for e in u]
                x = [mod_x[0] * e for e in u]
                y = [mod_y[0] * e for e in u]
                z = [mod_low[0] * e for e in u]
                for v in range(1, KL + 1):
                    up_row = rows_ref[s, v - 1]
                    down_row = rows_ref[s, KL + v - 1]
                    up_weight, down_weight = weight_ref[s, v - 1], weight_ref[s, KL + v - 1]
                    m, mx, my, mz = mod[v], mod_x[v], mod_y[v], mod_low[v]
                    for c in range(3):
                        e = up_weight * gathered[pl.ds(up_row + c * ROW, 8), :]
                        e = e + down_weight * gathered[pl.ds(down_row + c * ROW, 8), :]
                        at[c] = at[c] + m * e
                        x[c] = x[c] + mx * e
                        y[c] = y[c] + my * e
                        z[c] = z[c] + mz * e
                own_part(i, g, j, at, x, y, z)
            send(turn, 0, g)
            return 0

        lax.fori_loop(0, GROUPS, couple, 0)

        def first_update(g, _):
            receive(turn, 0, g)
            i, _, _ = exchange(turn, 0, g)
            for j in range(GSLOTS):
                image = minus_image(i, g, j)
                starts = []
                for c in range(3):
                    r = f_ref[slot_rows(g, j, c, 8), :] + image[c]
                    z = r * (1.0 / THETA)
                    rows = slot_rows(g, j, c, ROW)
                    r_ref[rows, :] = r[:ROW]
                    z_ref[rows, :] = z[:ROW]
                    p_ref[rows, :] = z[:ROW]
                    starts.append(jnp.where(inside, z, 0.0))
                mean_part(turn, 1, g, j, starts)
            send(turn, 1, g)
            return 0

        lax.fori_loop(0, GROUPS, first_update, 0)

        for k in range(1, SWEEPS + 1):
            keep, gain = factors[k - 1]

            def sweep(g, _, k=k, keep=keep, gain=gain):
                receive(turn, k, g)
                i, _, _ = exchange(turn, k, g)
                for j in range(GSLOTS):
                    image = minus_image(i, g, j)
                    updated = []
                    for c in range(3):
                        whole, rows = slot_rows(g, j, c, 8), slot_rows(g, j, c, ROW)
                        p = keep * p_ref[whole, :] + gain * (r_ref[whole, :] + image[c])
                        z = z_ref[whole, :] + p
                        if k < SWEEPS:
                            p_ref[rows, :] = p[:ROW]
                            z_ref[rows, :] = z[:ROW]
                            updated.append(jnp.where(inside, z, 0.0))
                        else:
                            u_ref[rows, :] = (u_ref[whole, :] + z)[:ROW]
                    if k < SWEEPS:
                        mean_part(turn, k + 1, g, j, updated)
                if k < SWEEPS:
                    send(turn, k + 1, g)
                return 0

            lax.fori_loop(0, GROUPS, sweep, 0)

    for turn in range(ITERS):
        iteration(turn)

    def give(s, _):
        for c in range(3):
            for k in range(ROW):
                at = pl.ds(s * PER_SLOT + c * ROW + k, 1)
                sol_ref[s, c : c + 1, 128 * k : 128 * k + 128] = u_ref[at, :]
                res_ref[s, c : c + 1, 128 * k : 128 * k + 128] = r_ref[at, :]
        return 0

    lax.fori_loop(0, SLOTS_DEV, give, 0)

    @pl.when(has_high)
    def _():
        mod_copy.wait_send()

    for turn in range(ITERS):
        for kind, message in steps:
            if kind == "send":
                gather_copy(turn, kind, message).wait_send()
        for k in range(SWEEPS + 1):
            for g in range(GROUPS):
                sent(turn, k, g)


def per_device(displacement, load, mean_modulus, modes, owner):
    rows, weights = neighbour_tables(owner)
    messages = sum(kind == "wait" for kind, _ in gather_plan())
    exchanges = ITERS * (SWEEPS + 1) * GROUPS
    field = pltpu.VMEM((BLOCK, 128), jnp.float32)
    moduli_field = pltpu.VMEM((KL + 1, 8, 128), jnp.float32)
    planes = pltpu.VMEM((exchanges, GROWS, 128), jnp.float32)
    out = jax.ShapeDtypeStruct(displacement.shape, jnp.float32)
    smem, vmem = pl.BlockSpec(memory_space=pltpu.SMEM), pl.BlockSpec(memory_space=pltpu.VMEM)
    dma = pltpu.SemaphoreType.DMA
    return pl.pallas_call(
        kernel,
        out_shape=(out, out),
        in_specs=[smem, smem, vmem, vmem, vmem, vmem],
        out_specs=(vmem, vmem),
        scratch_shapes=[
            pltpu.VMEM((PX * PY * BLOCK, 128), jnp.float32),
            pltpu.VMEM((PX * PY * BLOCK, 128), jnp.float32),
            field,
            field,
            field,
            field,
            field,
            field,
            moduli_field,
            moduli_field,
            moduli_field,
            moduli_field,
            planes,
            planes,
            planes,
            planes,
            dma((ITERS, messages)),
            dma((ITERS, messages)),
            dma((exchanges,)),
            dma((exchanges,)),
            dma((exchanges,)),
            dma((exchanges,)),
            dma,
            dma,
        ],
        compiler_params=pltpu.CompilerParams(collective_id=0, has_side_effects=True),
        name="galerkin",
    )(rows, weights, displacement, load, mean_modulus, modes)


def solution(mesh):
    in_specs = (P("chaos", None, "slab"), P("chaos", None, "slab"), P("slab"), P(None, "slab"), P())
    out_specs = (P("chaos", None, "slab"), P("chaos", None, "slab"))
    return jax.shard_map(
        per_device, mesh=mesh, in_specs=in_specs, out_specs=out_specs, check_vma=False
    )
```

```python
import functools
import heapq
import itertools
import math

import jax
import jax.numpy as jnp
import numpy as np
from jax import lax
from jax.experimental import pallas as pl
from jax.experimental.pallas import tpu as pltpu
from jax.sharding import PartitionSpec as P

NX, NY, KL, DEG, SWEEPS, ITERS = 24, 32, 10, 3, 4, 2
PX, PY = 4, 8
SLOTS_DEV = 9
ROW = 6
PER_SLOT = 3 * ROW
BLOCK = 168
GROUPS = 3
GSLOTS = SLOTS_DEV // GROUPS
GROWS = 56
THETA, DELTA = 26.25, 23.75
MESH = pl.DeviceIdType.MESH
DIRS = {"x+": (1, 0), "x-": (-1, 0), "y+": (0, 1), "y-": (0, -1)}
CHUNKS = (("x", 0, 64, 32), ("y", 64, 104, 56))
MODES = {("x", 0): "leap", ("y", 0): "leap", ("x", 1): "chain", ("y", 1): "chain"}
LATENCY, HOP, RATE, AHEAD = 3.4, 0.8, 80.0, 1.2


def piece_rows(chunk, half):
    _, first, size, upper = CHUNKS[chunk]
    return {None: (first, size), 0: (first, upper), 1: (first + upper, size - upper)}[half]


def relative(ox, oy):
    return ((ox + PX // 2 - 1) % PX - (PX // 2 - 1), (oy + PY // 2 - 1) % PY - (PY // 2 - 1))


def onward(axis, stage, reach):
    far = (PX if axis == "x" else PY) // 2
    if MODES[axis, stage] == "chain":
        return [(1, reach == far - 1)] if reach < far else []
    if far == 2:
        return [(1, False), (2, True)] if reach == 0 else []
    return {0: [(1, False), (2, False)], 2: [(1, False), (2, True)]}.get(reach, [])


def depth(axis, stage, reach):
    return max((1 + depth(axis, stage, reach + hops) for hops, _ in onward(axis, stage, reach)), default=0)


def gather_plan():
    count = itertools.count()
    halves = {}

    def carried(way, chunk, owner, stage):
        reach = abs(owner["xy".index(way[0])])
        return [
            (way, hops, chunk, owner, (0 if way[1] == "+" else 1) if half else None)
            for hops, half in onward(way[0], stage, reach)
        ]

    def allowed(way, chunk, owner, half):
        first = CHUNKS[chunk][0]
        if way[0] != first:
            return carried(way, chunk, owner, 1)
        sends = carried(way, chunk, owner, 0) if half is None else []
        if half is not None:
            halves[chunk, owner] = halves.get((chunk, owner), 0) + 1
        if half is None or halves[chunk, owner] == 2:
            second = "y" if first == "x" else "x"
            for sign in "+-":
                sends += carried(second + sign, chunk, owner, 1)
        return sends

    def urgency(message):
        way, hops, chunk, owner, _ = message
        axis, first = way[0], CHUNKS[chunk][0]
        reach = abs(owner["xy".index(axis)]) + hops
        if axis != first:
            return -depth(axis, 1, reach)
        return -depth(axis, 0, reach) - depth("y" if axis == "x" else "x", 1, 0)

    queues, busy = {d: [] for d in DIRS}, dict.fromkeys(DIRS, False)
    events, steps = [], []

    def put(message, now):
        heapq.heappush(queues[message[0]], (urgency(message), next(count), message, now))

    def begin(way, now):
        if queues[way] and not busy[way]:
            _, _, message, since = heapq.heappop(queues[way])
            busy[way] = True
            steps.append((max(since, now - AHEAD), next(count), "send", message))
            hops = message[1]
            took = hops * piece_rows(message[2], message[4])[1] / RATE
            heapq.heappush(events, (now + took, next(count), "sent", message))
            here = now + took + LATENCY + HOP * (hops - 1)
            heapq.heappush(events, (here, next(count), "here", message))

    for stage in (0, 1):
        for sign in "+-":
            for chunk, (first, *_) in enumerate(CHUNKS):
                axis = first if stage == 0 else "y" if first == "x" else "x"
                for message in carried(axis + sign, chunk, (0, 0), stage):
                    put(message, 0.0)
    for way in DIRS:
        begin(way, 0.0)
    while events:
        now, _, kind, message = heapq.heappop(events)
        way, hops, chunk, owner, half = message
        if kind == "sent":
            busy[way] = False
        else:
            dx, dy = DIRS[way]
            owner = relative(owner[0] - dx * hops, owner[1] - dy * hops)
            steps.append((now, next(count), "wait", (way, hops, chunk, owner, half)))
            for message in allowed(way, chunk, owner, half):
                put(message, now)
        for each in DIRS:
            begin(each, now)
    return [(kind, message) for _, _, kind, message in sorted(steps)]


def multi_indices():
    listing = [[]]
    for variable in range(KL):
        extended = []
        for prefix in listing:
            for degree in range(DEG + 1 - sum(prefix)):
                extended.append(prefix + [degree])
        listing = extended
    return listing


def chaos_tables(slots_all):
    listing = multi_indices()
    lookup = {tuple(entry): number for number, entry in enumerate(listing)}
    packed = np.zeros((2 * KL + 1, slots_all), np.int32)
    packed[2 * KL, : len(listing)] = 1
    for number, entry in enumerate(listing):
        for variable in range(KL):
            for side, step in ((0, 1), (1, -1)):
                other = list(entry)
                other[variable] += step
                if tuple(other) in lookup:
                    square = max(entry[variable], other[variable])
                    packed[side * KL + variable, number] = 4 * (lookup[tuple(other)] + 1) + square
    return packed


def neighbour_tables(owner):
    slots_all = owner.shape[0]
    own = lax.dynamic_slice_in_dim(owner, lax.axis_index("chaos") * SLOTS_DEV, SLOTS_DEV, 0)
    numbers = jnp.arange(slots_all, dtype=jnp.int32)
    chosen = own[:, None, None] == numbers
    packed = jnp.sum(jnp.where(chosen, jnp.asarray(chaos_tables(slots_all)), 0), axis=-1)
    rows = 4 * ((numbers // SLOTS_DEV) * BLOCK + (numbers % SLOTS_DEV) * PER_SLOT)
    found = (packed // 4)[:, :, None] == owner + 1
    return jnp.sum(jnp.where(found, rows, 0), axis=-1) + packed % 4


def kernel(
    rows_ref,
    disp_ref,
    load_ref,
    mean_ref,
    modes_ref,
    sol_ref,
    res_ref,
    row_of,
    weight_of,
    gathered_0,
    gathered_1,
    u_ref,
    f_ref,
    r_ref,
    z_ref,
    p_ref,
    t_ref,
    mod,
    mod_low,
    mod_x,
    mod_y,
    up_out,
    down_out,
    up_in,
    down_in,
    ag_send,
    ag_recv,
    up_send,
    up_recv,
    down_send,
    down_recv,
    mod_send,
    mod_recv,
):
    chaos = lax.axis_index("chaos")
    slab = lax.axis_index("slab")
    slabs = lax.axis_size("slab")
    cx, cy = chaos // PY, chaos % PY
    has_low, has_high = slab > 0, slab < slabs - 1

    def unpack(s, _):
        for n in range(2 * KL):
            entry = rows_ref[s, n]
            square = lax.rem(entry, 4)
            small = jnp.where(square == 1, 1.0, 0.0)
            large = jnp.where(square == 2, math.sqrt(2.0), math.sqrt(3.0))
            row_of[s, n] = lax.div(entry, 4)
            weight_of[s, n] = jnp.where(square < 2, small, large)
        return 0

    def chaos_at(dx, dy):
        return lax.rem(cx + dx + PX, PX) * PY + lax.rem(cy + dy + PY, PY)

    lane = lax.broadcasted_iota(jnp.int32, (8, 128), 1)
    sub = lax.broadcasted_iota(jnp.int32, (8, 128), 0)
    inside = sub < ROW
    first_y = lane % NY == 0
    zero = jnp.zeros((8, 128), jnp.float32)

    def up_x(f):
        rolled = pltpu.roll(f, 128 - NY, 1)
        return jnp.where(lane < 128 - NY, rolled, pltpu.roll(rolled, 7, 0))

    def down_x(f):
        rolled = pltpu.roll(f, NY, 1)
        return jnp.where(lane < NY, pltpu.roll(rolled, 1, 0), rolled)

    def up_y(f):
        return pltpu.roll(f, 127, 1)

    def down_y(f):
        return jnp.where(first_y, 0.0, pltpu.roll(f, 1, 1))

    barrier = pltpu.get_barrier_semaphore()
    peers = [*DIRS.values(), (2, 0), (0, 2), (0, -2)]
    for dx, dy in peers:
        pl.semaphore_signal(
            barrier, inc=1, device_id=(chaos_at(dx, dy), slab), device_id_type=MESH
        )

    @pl.when(has_low)
    def _():
        pl.semaphore_signal(barrier, inc=1, device_id=(chaos, slab - 1), device_id_type=MESH)

    @pl.when(has_high)
    def _():
        pl.semaphore_signal(barrier, inc=1, device_id=(chaos, slab + 1), device_id_type=MESH)

    for ref in (u_ref, z_ref):
        ref[BLOCK - 8 : BLOCK, :] = zero

    def take(s, _):
        live = rows_ref[s, 2 * KL] == 1
        for c in range(3):
            for k in range(ROW):
                at = pl.ds(s * PER_SLOT + c * ROW + k, 1)
                piece = disp_ref[s, c : c + 1, 128 * k : 128 * k + 128]
                u_ref[at, :] = jnp.where(live, piece, 0.0)
                piece = load_ref[s, c : c + 1, 128 * k : 128 * k + 128]
                f_ref[at, :] = jnp.where(live, piece, 0.0)
        return 0

    lax.fori_loop(0, SLOTS_DEV, take, 0)
    for v in range(KL + 1):
        mod[v] = zero
        for k in range(ROW):
            nodes = slice(128 * k, 128 * k + 128)
            if v == 0:
                mod[0, k, :] = mean_ref[nodes]
            else:
                mod[v, k : k + 1, :] = modes_ref[v - 1 : v, nodes]

    @pl.when(jnp.logical_not(has_low))
    def _():
        for v in range(KL + 1):
            mod_low[v] = zero

        def clear(i, _):
            up_in[i] = jnp.zeros((GROWS, 128), jnp.float32)
            return 0

        lax.fori_loop(0, ITERS * (SWEEPS + 1) * GROUPS, clear, 0)

    @pl.when(jnp.logical_not(has_high))
    def _():
        def clear(i, _):
            down_in[i] = jnp.zeros((GROWS, 128), jnp.float32)
            return 0

        lax.fori_loop(0, ITERS * (SWEEPS + 1) * GROUPS, clear, 0)

    neighbours = len(peers) + has_low.astype(jnp.int32) + has_high.astype(jnp.int32)
    pl.semaphore_wait(barrier, neighbours)

    mod_copy = pltpu.make_async_remote_copy(
        src_ref=mod,
        dst_ref=mod_low,
        send_sem=mod_send,
        recv_sem=mod_recv,
        device_id=(chaos, slab + 1),
        device_id_type=MESH,
    )

    @pl.when(has_high)
    def _():
        mod_copy.start()

    blocks = (gathered_0, gathered_1)
    steps = gather_plan()
    waits = [message for kind, message in steps if kind == "wait"]
    ids = {message: number for number, message in enumerate(waits)}

    def gather_copy(turn, kind, message):
        way, hops, chunk, owner, half = message
        dx, dy = (hops * d for d in DIRS[way])
        if kind == "send":
            message = (way, hops, chunk, relative(owner[0] - dx, owner[1] - dy), half)
        number = ids[message]
        first, size = piece_rows(chunk, half)
        base = chaos_at(*owner) * BLOCK + first
        piece = blocks[turn].at[pl.ds(pl.multiple_of(base, 8), size)]
        return pltpu.make_async_remote_copy(
            src_ref=piece,
            dst_ref=piece,
            send_sem=ag_send.at[turn, number],
            recv_sem=ag_recv.at[turn, number],
            device_id=(chaos_at(dx, dy), slab),
            device_id_type=MESH,
        )

    def exchange(turn, k, g):
        i = (turn * (SWEEPS + 1) + k) * GROUPS + g
        up = pltpu.make_async_remote_copy(
            src_ref=up_out.at[i],
            dst_ref=up_in.at[i],
            send_sem=up_send.at[i],
            recv_sem=up_recv.at[i],
            device_id=(chaos, slab + 1),
            device_id_type=MESH,
        )
        down = pltpu.make_async_remote_copy(
            src_ref=down_out.at[i],
            dst_ref=down_in.at[i],
            send_sem=down_send.at[i],
            recv_sem=down_recv.at[i],
            device_id=(chaos, slab - 1),
            device_id_type=MESH,
        )
        return i, up, down

    def send(turn, k, g):
        _, up, down = exchange(turn, k, g)

        @pl.when(has_high)
        def _():
            up.start()

        @pl.when(has_low)
        def _():
            down.start()

    def receive(turn, k, g):
        _, up, down = exchange(turn, k, g)

        @pl.when(has_low)
        def _():
            up.wait_recv()

        @pl.when(has_high)
        def _():
            down.wait_recv()

    def sent(turn, k, g):
        _, up, down = exchange(turn, k, g)

        @pl.when(has_high)
        def _():
            up.wait_send()

        @pl.when(has_low)
        def _():
            down.wait_send()

    def own_part(i, g, j, at, x, y, z):
        px, py = [up_x(e) for e in x], [up_y(e) for e in y]
        spread = (px[0] - at[0]) + (py[1] - at[1]) - at[2]
        flux_x = [px[c] - at[c] for c in range(3)]
        flux_y = [py[c] - at[c] for c in range(3)]
        flux_x[0] = flux_x[0] + spread
        flux_y[1] = flux_y[1] + spread
        base = (g * GSLOTS + j) * PER_SLOT
        for c in range(3):
            total = (flux_x[c] - down_x(flux_x[c])) + (flux_y[c] - down_y(flux_y[c]))
            total = total - at[c] - z[c]
            if c == 2:
                total = total + spread - z[c]
            t_ref[pl.ds(base + c * ROW, ROW), :] = total[:ROW]
            low = at[c] if c < 2 else at[c] - spread
            inner = pl.ds(j * PER_SLOT + c * ROW, ROW)
            up_out[i, inner, :] = low[:ROW]
            down_out[i, inner, :] = z[c][:ROW]

    def minus_image(i, g, j):
        base = (g * GSLOTS + j) * PER_SLOT
        low = [up_in[i, pl.ds(j * PER_SLOT + c * ROW, 8), :] for c in range(3)]
        high = [down_in[i, pl.ds(j * PER_SLOT + c * ROW, 8), :] for c in range(3)]
        across = jnp.where(inside, high[2], 0.0)
        own = [t_ref[pl.ds(base + c * ROW, 8), :] for c in range(3)]
        return [
            own[0] + (across - down_x(across)) + high[0] + low[0],
            own[1] + (across - down_y(across)) + high[1] + low[1],
            own[2] + 2.0 * across + low[2],
        ]

    def slot_rows(g, j, c, size):
        return pl.ds((g * GSLOTS + j) * PER_SLOT + c * ROW, size)

    def mean_part(turn, k, g, j, z):
        i, _, _ = exchange(turn, k, g)
        own_part(
            i,
            g,
            j,
            [mod[0] * e for e in z],
            [mod_x[0] * e for e in z],
            [mod_y[0] * e for e in z],
            [mod_low[0] * e for e in z],
        )

    ratio = THETA / DELTA
    rho = 1.0 / ratio
    factors = []
    for _ in range(SWEEPS):
        rho_next = 1.0 / (2.0 * ratio - rho)
        factors.append((rho_next * rho, 2.0 * rho_next / DELTA))
        rho = rho_next

    def iteration(turn):
        gathered = blocks[turn]
        gathered[pl.ds(pl.multiple_of(chaos * BLOCK, 8), BLOCK), :] = u_ref[...]
        began = steps.index(next(step for step in steps if step[0] == "wait"))
        for kind, message in steps[:began]:
            gather_copy(turn, kind, message).start()

        if turn == 0:
            lax.fori_loop(0, SLOTS_DEV, unpack, 0)

            @pl.when(has_low)
            def _():
                mod_copy.wait_recv()

            for v in range(KL + 1):
                mod_x[v] = jnp.where(inside, down_x(mod[v]), 0.0)
                mod_y[v] = down_y(mod[v])

        for kind, message in steps[began:]:
            if kind == "send":
                gather_copy(turn, kind, message).start()
            else:
                gather_copy(turn, kind, message).wait_recv()

        def couple(g, _):
            i, _, _ = exchange(turn, 0, g)
            for j in range(GSLOTS):
                s = g * GSLOTS + j
                u = [u_ref[slot_rows(g, j, c, 8), :] for c in range(3)]
                at = [mod[0] * e for e in u]
                x = [mod_x[0] * e for e in u]
                y = [mod_y[0] * e for e in u]
                z = [mod_low[0] * e for e in u]
                for v in range(1, KL + 1):
                    up_row, up_weight = row_of[s, v - 1], weight_of[s, v - 1]
                    down_row, down_weight = row_of[s, KL + v - 1], weight_of[s, KL + v - 1]
                    m, mx, my, mz = mod[v], mod_x[v], mod_y[v], mod_low[v]
                    for c in range(3):
                        e = up_weight * gathered[pl.ds(up_row + c * ROW, 8), :]
                        e = e + down_weight * gathered[pl.ds(down_row + c * ROW, 8), :]
                        at[c] = at[c] + m * e
                        x[c] = x[c] + mx * e
                        y[c] = y[c] + my * e
                        z[c] = z[c] + mz * e
                own_part(i, g, j, at, x, y, z)
            send(turn, 0, g)
            return 0

        lax.fori_loop(0, GROUPS, couple, 0)

        def first_update(g, _):
            receive(turn, 0, g)
            i, _, _ = exchange(turn, 0, g)
            for j in range(GSLOTS):
                image = minus_image(i, g, j)
                starts = []
                for c in range(3):
                    r = f_ref[slot_rows(g, j, c, 8), :] + image[c]
                    z = r * (1.0 / THETA)
                    rows = slot_rows(g, j, c, ROW)
                    r_ref[rows, :] = r[:ROW]
                    z_ref[rows, :] = z[:ROW]
                    p_ref[rows, :] = z[:ROW]
                    starts.append(jnp.where(inside, z, 0.0))
                mean_part(turn, 1, g, j, starts)
            send(turn, 1, g)
            return 0

        lax.fori_loop(0, GROUPS, first_update, 0)

        for k in range(1, SWEEPS + 1):
            keep, gain = factors[k - 1]

            def sweep(g, _, k=k, keep=keep, gain=gain):
                receive(turn, k, g)
                i, _, _ = exchange(turn, k, g)
                for j in range(GSLOTS):
                    image = minus_image(i, g, j)
                    updated = []
                    for c in range(3):
                        whole, rows = slot_rows(g, j, c, 8), slot_rows(g, j, c, ROW)
                        p = keep * p_ref[whole, :] + gain * (r_ref[whole, :] + image[c])
                        z = z_ref[whole, :] + p
                        if k < SWEEPS:
                            p_ref[rows, :] = p[:ROW]
                            z_ref[rows, :] = z[:ROW]
                            updated.append(jnp.where(inside, z, 0.0))
                        else:
                            u_ref[rows, :] = (u_ref[whole, :] + z)[:ROW]
                    if k < SWEEPS:
                        mean_part(turn, k + 1, g, j, updated)
                if k < SWEEPS:
                    send(turn, k + 1, g)
                return 0

            lax.fori_loop(0, GROUPS, sweep, 0)

    for turn in range(ITERS):
        iteration(turn)

    def give(s, _):
        for c in range(3):
            for k in range(ROW):
                at = pl.ds(s * PER_SLOT + c * ROW + k, 1)
                sol_ref[s, c : c + 1, 128 * k : 128 * k + 128] = u_ref[at, :]
                res_ref[s, c : c + 1, 128 * k : 128 * k + 128] = r_ref[at, :]
        return 0

    lax.fori_loop(0, SLOTS_DEV, give, 0)

    @pl.when(has_high)
    def _():
        mod_copy.wait_send()

    for turn in range(ITERS):
        for kind, message in steps:
            if kind == "send":
                gather_copy(turn, kind, message).wait_send()
        for k in range(SWEEPS + 1):
            for g in range(GROUPS):
                sent(turn, k, g)


def per_device(displacement, load, mean_modulus, modes, owner):
    rows = neighbour_tables(owner)
    messages = sum(kind == "wait" for kind, _ in gather_plan())
    exchanges = ITERS * (SWEEPS + 1) * GROUPS
    field = pltpu.VMEM((BLOCK, 128), jnp.float32)
    moduli_field = pltpu.VMEM((KL + 1, 8, 128), jnp.float32)
    planes = pltpu.VMEM((exchanges, GROWS, 128), jnp.float32)
    out = jax.ShapeDtypeStruct(displacement.shape, jnp.float32)
    smem, vmem = pl.BlockSpec(memory_space=pltpu.SMEM), pl.BlockSpec(memory_space=pltpu.VMEM)
    dma = pltpu.SemaphoreType.DMA
    return pl.pallas_call(
        kernel,
        out_shape=(out, out),
        in_specs=[smem, vmem, vmem, vmem, vmem],
        out_specs=(vmem, vmem),
        scratch_shapes=[
            pltpu.SMEM((SLOTS_DEV, 2 * KL), jnp.int32),
            pltpu.SMEM((SLOTS_DEV, 2 * KL), jnp.float32),
            pltpu.VMEM((PX * PY * BLOCK, 128), jnp.float32),
            pltpu.VMEM((PX * PY * BLOCK, 128), jnp.float32),
            field,
            field,
            field,
            field,
            field,
            field,
            moduli_field,
            moduli_field,
            moduli_field,
            moduli_field,
            planes,
            planes,
            planes,
            planes,
            dma((ITERS, messages)),
            dma((ITERS, messages)),
            dma((exchanges,)),
            dma((exchanges,)),
            dma((exchanges,)),
            dma((exchanges,)),
            dma,
            dma,
        ],
        compiler_params=pltpu.CompilerParams(collective_id=0, has_side_effects=True),
        name="galerkin",
    )(rows, displacement, load, mean_modulus, modes)


def solution(mesh):
    in_specs = (P("chaos", None, "slab"), P("chaos", None, "slab"), P("slab"), P(None, "slab"), P())
    out_specs = (P("chaos", None, "slab"), P("chaos", None, "slab"))
    return jax.shard_map(
        per_device, mesh=mesh, in_specs=in_specs, out_specs=out_specs, check_vma=False
    )
```
